8 devices in a mesh: fsdp: 8 (over z, y, x, core).
Axes of the slice: x: 2, y: 2, z: 1, core: 2. Of those that a mesh axis runs over, the one named last changes fastest.
Arguments:
- token_ids: int32 [16, 512], P('fsdp')
- grad_y: bfloat16 [16, 512, 2048], P('fsdp')
- table: bfloat16 [128256, 2048], P('fsdp')
- norm1_gain: bfloat16 [2048], P('fsdp')
- norm2_gain: bfloat16 [2048], P('fsdp')
- w_query: bfloat16 [2048, 32, 64], P('fsdp')
- w_key: bfloat16 [2048, 8, 64], P('fsdp')
- w_value: bfloat16 [2048, 8, 64], P('fsdp')
- w_out: bfloat16 [2048, 2048], P('fsdp')
- w_gate: bfloat16 [2048, 8192], P('fsdp')
- w_up: bfloat16 [2048, 8192], P('fsdp')
- w_down: bfloat16 [8192, 2048], P('fsdp')
Outputs:
- output 1: bfloat16 [16, 512, 2048], P('fsdp')
- output 2: bfloat16 [128256, 2048], P('fsdp')
- output 3: bfloat16 [2048], P('fsdp')
- output 4: bfloat16 [2048], P('fsdp')
- output 5: bfloat16 [2048, 32, 64], P('fsdp')
- output 6: bfloat16 [2048, 8, 64], P('fsdp')
- output 7: bfloat16 [2048, 8, 64], P('fsdp')
- output 8: bfloat16 [2048, 2048], P('fsdp')
- output 9: bfloat16 [2048, 8192], P('fsdp')
- output 10: bfloat16 [2048, 8192], P('fsdp')
- output 11: bfloat16 [8192, 2048], P('fsdp')
All inputs are finite; a program needn't handle non-finite values.
Results may differ from the reference program's by a relative error of at most 0.015642.
Values are sent between devices in bfloat16 or wider.
A program may use at most 1 GiB of HBM per device.

```python
import jax
import jax.numpy as jnp
from jax import lax

VOCAB_SIZE = 128256
MODEL_DIM = 2048
Q_HEADS = 32
KV_HEADS = 8
HEAD_DIM = 64
FFN_DIM = 8192
GLOBAL_BATCH = 16
SEQ_LEN = 512

NORM_EPS = 1e-5
ROPE_THETA = 500000.0
VOCAB_BITS = (VOCAB_SIZE - 1).bit_length()
TOKENS_ALL = GLOBAL_BATCH * SEQ_LEN


def draw_ids(rng_key):
    k_level, k_rank, k_flat, k_pick, k_perm = jax.random.split(rng_key, 5)
    id_shape = (GLOBAL_BATCH, SEQ_LEN)
    levels = jax.random.randint(k_level, id_shape, 0, VOCAB_BITS + 1)
    level_span = jnp.minimum(jnp.left_shift(jnp.ones(id_shape, jnp.int32), levels), VOCAB_SIZE)
    id_ranks = jax.random.randint(k_rank, id_shape, 0, level_span)
    flat_ids = jax.random.randint(k_flat, id_shape, 0, VOCAB_SIZE)
    use_flat = jax.random.randint(k_pick, id_shape, 0, 4) == 0
    id_ranks = jnp.where(use_flat, flat_ids, id_ranks)
    row_order = jax.random.permutation(k_perm, VOCAB_SIZE)
    return jnp.take(row_order, id_ranks).astype(jnp.int32)


def normal_weight(rng_key, w_shape, fan_in):
    return (jax.random.normal(rng_key, w_shape, jnp.float32) * fan_in ** -0.5).astype(jnp.bfloat16)


def setup_inputs(seed: int = 0) -> dict:
    keys = jax.random.split(jax.random.key(seed), 12)
    attn_width = Q_HEADS * HEAD_DIM
    return {
        "token_ids": draw_ids(keys[0]),
        "grad_y": (jax.random.normal(keys[1], (GLOBAL_BATCH, SEQ_LEN, MODEL_DIM), jnp.float32) * TOKENS_ALL ** -0.5).astype(jnp.bfloat16),
        "table": jax.random.normal(keys[2], (VOCAB_SIZE, MODEL_DIM), jnp.float32).astype(jnp.bfloat16),
        "norm1_gain": jax.random.uniform(keys[3], (MODEL_DIM,), jnp.float32, 0.5, 1.5).astype(jnp.bfloat16),
        "norm2_gain": jax.random.uniform(keys[4], (MODEL_DIM,), jnp.float32, 0.5, 1.5).astype(jnp.bfloat16),
        "w_query": normal_weight(keys[5], (MODEL_DIM, Q_HEADS, HEAD_DIM), MODEL_DIM),
        "w_key": normal_weight(keys[6], (MODEL_DIM, KV_HEADS, HEAD_DIM), MODEL_DIM),
        "w_value": normal_weight(keys[7], (MODEL_DIM, KV_HEADS, HEAD_DIM), MODEL_DIM),
        "w_out": normal_weight(keys[8], (attn_width, MODEL_DIM), attn_width),
        "w_gate": normal_weight(keys[9], (MODEL_DIM, FFN_DIM), MODEL_DIM),
        "w_up": normal_weight(keys[10], (MODEL_DIM, FFN_DIM), MODEL_DIM),
        "w_down": normal_weight(keys[11], (FFN_DIM, MODEL_DIM), FFN_DIM),
    }


def rms_norm(x_f32, gain_f32):
    inv_rms = lax.rsqrt(jnp.mean(x_f32 * x_f32, axis=-1, keepdims=True) + NORM_EPS)
    return (x_f32 * inv_rms * gain_f32).astype(jnp.bfloat16)


def rotary(x_f32):
    head_dim = x_f32.shape[-1]
    half_dim = head_dim // 2
    seq_len = x_f32.shape[-3]
    inv_freq = ROPE_THETA ** (-2.0 * jnp.arange(half_dim, dtype=jnp.float32) / head_dim)
    angles = jnp.arange(seq_len, dtype=jnp.float32)[:, None] * inv_freq[None, :]
    cos_tab = jnp.cos(angles)[:, None, :]
    sin_tab = jnp.sin(angles)[:, None, :]
    lo_half = x_f32[..., :half_dim]
    hi_half = x_f32[..., half_dim:]
    return jnp.concatenate([lo_half * cos_tab - hi_half * sin_tab, hi_half * cos_tab + lo_half * sin_tab], axis=-1)


def attend(q_f32, k_f32, v_bf16):
    q_rot = rotary(q_f32).astype(jnp.bfloat16).reshape(SEQ_LEN, KV_HEADS, Q_HEADS // KV_HEADS, HEAD_DIM)
    k_rot = rotary(k_f32).astype(jnp.bfloat16)
    scores = jnp.einsum("qkgd,skd->kgqs", q_rot.astype(jnp.float32), k_rot.astype(jnp.float32)) * HEAD_DIM ** -0.5
    positions = jnp.arange(SEQ_LEN)
    causal = positions[:, None] >= positions[None, :]
    scores = jnp.where(causal, scores, -1e30)
    prob_bf = jax.nn.softmax(scores, axis=-1).astype(jnp.bfloat16)
    attn_out = jnp.einsum("kgqs,skd->qkgd", prob_bf.astype(jnp.float32), v_bf16.astype(jnp.float32))
    return attn_out.astype(jnp.bfloat16).reshape(SEQ_LEN, Q_HEADS * HEAD_DIM)


def layer(emb_rows, gain_one, gain_two, w_query, w_key, w_value, w_out, w_gate, w_up, w_down):
    x_f32 = emb_rows.astype(jnp.float32)
    h_one = rms_norm(x_f32, gain_one).astype(jnp.float32)
    q_f32 = jnp.einsum("sd,dhe->she", h_one, w_query)
    k_f32 = jnp.einsum("sd,dhe->she", h_one, w_key)
    v_bf16 = jnp.einsum("sd,dhe->she", h_one, w_value).astype(jnp.bfloat16)
    attn_out = attend(q_f32, k_f32, v_bf16)
    resid_f32 = x_f32 + jnp.dot(attn_out.astype(jnp.float32), w_out, preferred_element_type=jnp.float32)
    resid_two = resid_f32.astype(jnp.bfloat16).astype(jnp.float32)
    h_two = rms_norm(resid_two, gain_two).astype(jnp.float32)
    gate_f32 = jnp.dot(h_two, w_gate, preferred_element_type=jnp.float32)
    up_f32 = jnp.dot(h_two, w_up, preferred_element_type=jnp.float32)
    act_f32 = (jax.nn.silu(gate_f32) * up_f32).astype(jnp.bfloat16).astype(jnp.float32)
    return (resid_two + jnp.dot(act_f32, w_down, preferred_element_type=jnp.float32)).astype(jnp.bfloat16)


def reference(token_ids, grad_y, table, norm1_gain, norm2_gain, w_query, w_key, w_value, w_out, w_gate, w_up, w_down):
    params = tuple(weight.astype(jnp.float32) for weight in (norm1_gain, norm2_gain, w_query, w_key, w_value, w_out, w_gate, w_up, w_down))

    def one_sequence(grad_acc, seq_in):
        seq_ids, seq_dy = seq_in
        emb_rows = jnp.take(table, seq_ids, axis=0)
        layer_out, pullback = jax.vjp(layer, emb_rows, *params)
        cotangents = pullback(seq_dy)
        new_acc = tuple(acc_old + cot_new for acc_old, cot_new in zip(grad_acc, cotangents[1:]))
        return new_acc, (layer_out, cotangents[0])

    zero_acc = tuple(jnp.zeros_like(weight) for weight in params)
    grad_acc, (y_out, d_emb) = lax.scan(one_sequence, zero_acc, (token_ids, grad_y))
    grad_table = jax.ops.segment_sum(d_emb.reshape(-1, MODEL_DIM).astype(jnp.float32), token_ids.reshape(-1), num_segments=VOCAB_SIZE).astype(jnp.bfloat16)
    grads = [acc_val.astype(jnp.bfloat16) for acc_val in grad_acc]
    return (y_out, grad_table, grads[0], grads[1], grads[2], grads[3], grads[4], grads[5], grads[6], grads[7], grads[8])
```

```python
import functools

import jax
import jax.numpy as jnp
from jax import lax
from jax.experimental import pallas as pl
from jax.experimental.pallas import tpu as pltpu
from jax.sharding import PartitionSpec as P

AXIS_NAME = "fsdp"
NORM_EPS = 1e-5
ROPE_THETA = 500000.0
F32 = jnp.float32
BF16 = jnp.bfloat16

N_DEV = 8
BIT_CORE, BIT_X, BIT_Y = 1, 2, 4
SLOTS_FWD = 144
SLOTS_BWD = 288
GROUP = 8
TILE_ROWS = 512
CHUNK = 256


def swap(value, bit):
    return lax.ppermute(value, AXIS_NAME, [(i, i ^ bit) for i in range(N_DEV)])


def dot(a, b):
    return lax.dot_general(a, b, (((1,), (0,)), ((), ())), preferred_element_type=F32)


def dot_nt(a, b):
    return lax.dot_general(a, b, (((1,), (1,)), ((), ())), preferred_element_type=F32)


def dot_tn(a, b):
    return lax.dot_general(a, b, (((0,), (0,)), ((), ())), preferred_element_type=F32)


def rms_norm(x_f32, gain_f32):
    inv_rms = lax.rsqrt(jnp.mean(x_f32 * x_f32, axis=-1, keepdims=True) + NORM_EPS)
    return (x_f32 * inv_rms * gain_f32).astype(BF16)


def rotary(x_f32):
    head_dim = x_f32.shape[-1]
    half_dim = head_dim // 2
    seq_len = x_f32.shape[-3]
    inv_freq = ROPE_THETA ** (-2.0 * jnp.arange(half_dim, dtype=F32) / head_dim)
    angles = jnp.arange(seq_len, dtype=F32)[:, None] * inv_freq[None, :]
    cos_tab = jnp.cos(angles)[:, None, :]
    sin_tab = jnp.sin(angles)[:, None, :]
    lo_half = x_f32[..., :half_dim]
    hi_half = x_f32[..., half_dim:]
    return jnp.concatenate([lo_half * cos_tab - hi_half * sin_tab, hi_half * cos_tab + lo_half * sin_tab], axis=-1)


def attend(q_f32, k_f32, v_bf16):
    batch_loc, seq_len, q_heads, head_dim = q_f32.shape
    kv_heads = k_f32.shape[2]
    q_rot = rotary(q_f32).astype(BF16).reshape(batch_loc, seq_len, kv_heads, q_heads // kv_heads, head_dim)
    k_rot = rotary(k_f32).astype(BF16)
    scores = jnp.einsum("bqkgd,bskd->bkgqs", q_rot, k_rot, preferred_element_type=F32) * head_dim ** -0.5
    positions = jnp.arange(seq_len)
    causal = positions[:, None] >= positions[None, :]
    scores = jnp.where(causal, scores, -1e30)
    prob_bf = jax.nn.softmax(scores, axis=-1).astype(BF16)
    attn_out = jnp.einsum("bkgqs,bskd->bqkgd", prob_bf, v_bf16, preferred_element_type=F32)
    return attn_out.astype(BF16).reshape(batch_loc, seq_len, q_heads * head_dim)


def gated(gate_f32, up_f32):
    return (jax.nn.silu(gate_f32) * up_f32).astype(BF16)


def pick_kernel(rows_smem, count_smem, target_ref, table_ref, out_ref, held, sems):
    step = pl.program_id(0)
    slot = lax.rem(step, 2)
    slots = target_ref.shape[1]

    def issue(block, where):
        def body(s, carry):
            group = rows_smem[block * slots + s] // GROUP
            pltpu.make_async_copy(
                table_ref.at[pl.ds(pl.multiple_of(group * GROUP, GROUP), GROUP), :],
                held.at[where, s],
                sems.at[where],
            ).start()
            return carry

        lax.fori_loop(0, count_smem[block], body, 0)

    @pl.when(step == 0)
    def _():
        held[...] = jnp.zeros_like(held)
        issue(0, 0)

    @pl.when(step + 1 < pl.num_programs(0))
    def _():
        issue(step + 1, 1 - slot)

    def drain(s, carry):
        pltpu.make_async_copy(table_ref.at[pl.ds(0, GROUP), :], held.at[slot, 0], sems.at[slot]).wait()
        return carry

    lax.fori_loop(0, count_smem[step], drain, 0)
    lanes = lax.broadcasted_iota(jnp.int32, (slots, slots * GROUP), 1)
    select = (lanes == target_ref[0]).astype(F32).astype(BF16)
    rows = held[slot].reshape(slots * GROUP, held.shape[-1])
    out_ref[0] = jnp.dot(select, rows, preferred_element_type=F32).astype(BF16)


def pick_rows(table, rows, counts):
    blocks, slots = rows.shape
    width = table.shape[1]
    place = jnp.arange(slots, dtype=jnp.int32)[None, :]
    target = jnp.where(place < counts[:, None], place * GROUP + rows % GROUP, -1)[:, :, None]
    return pl.pallas_call(
        pick_kernel,
        out_shape=jax.ShapeDtypeStruct((blocks, slots, width), BF16),
        grid_spec=pltpu.PrefetchScalarGridSpec(
            num_scalar_prefetch=2,
            grid=(blocks,),
            in_specs=[
                pl.BlockSpec((1, slots, 1), lambda b, *_: (b, 0, 0)),
                pl.BlockSpec(memory_space=pl.ANY),
            ],
            out_specs=pl.BlockSpec((1, slots, width), lambda b, *_: (b, 0, 0)),
            scratch_shapes=[
                pltpu.VMEM((2, slots, GROUP, width), BF16),
                pltpu.SemaphoreType.DMA((2,)),
            ],
        ),
        compiler_params=pltpu.CompilerParams(vmem_limit_bytes=40 * 1024 * 1024),
        cost_estimate=pl.CostEstimate(flops=2 * blocks * slots * slots * GROUP * width, bytes_accessed=blocks * slots * GROUP * width * 2, transcendentals=0),
        name="pick_rows",
    )(rows.reshape(-1), counts, target, table)


def table_grad_kernel(first_smem, last_smem, ids_ref, rows_ref, out_ref, total):
    tile = pl.program_id(0)
    total[...] = jnp.zeros_like(total)
    base = tile * TILE_ROWS

    def body(c, carry):
        ids = ids_ref[pl.ds(c, 1), :]
        here = lax.broadcasted_iota(jnp.int32, (TILE_ROWS, CHUNK), 0) + base
        select = (here == ids).astype(F32).astype(BF16)
        rows = rows_ref[pl.ds(pl.multiple_of(c * CHUNK, CHUNK), CHUNK), :]
        total[...] += jnp.dot(select, rows, preferred_element_type=F32)
        return carry

    lax.fori_loop(first_smem[tile], last_smem[tile], body, 0)
    out_ref[...] = total[...].astype(BF16)


def table_grad(sorted_ids, sorted_rows, n_rows):
    count, width = sorted_rows.shape
    tiles = pl.cdiv(n_rows, TILE_ROWS)
    bounds = jnp.arange(tiles + 1, dtype=jnp.int32) * TILE_ROWS
    bounds = jnp.minimum(bounds, n_rows)
    below = jnp.sum((sorted_ids[None, :] < bounds[:, None]).astype(jnp.int32), axis=1)
    first = below[:-1] // CHUNK
    last = jnp.where(below[1:] > below[:-1], (below[1:] + CHUNK - 1) // CHUNK, first)
    return pl.pallas_call(
        table_grad_kernel,
        out_shape=jax.ShapeDtypeStruct((n_rows, width), BF16),
        grid_spec=pltpu.PrefetchScalarGridSpec(
            num_scalar_prefetch=2,
            grid=(tiles,),
            in_specs=[
                pl.BlockSpec((count // CHUNK, CHUNK), lambda t, *_: (0, 0)),
                pl.BlockSpec((count, width), lambda t, *_: (0, 0)),
            ],
            out_specs=pl.BlockSpec((TILE_ROWS, width), lambda t, *_: (t, 0)),
            scratch_shapes=[pltpu.VMEM((TILE_ROWS, width), F32)],
        ),
        compiler_params=pltpu.CompilerParams(vmem_limit_bytes=48 * 1024 * 1024),
        cost_estimate=pl.CostEstimate(flops=2 * 41 * TILE_ROWS * CHUNK * width, bytes_accessed=n_rows * width * 2, transcendentals=0),
        name="table_grad",
    )(first, last, sorted_ids.reshape(count // CHUNK, CHUNK), sorted_rows)


def solution(mesh):
    spec_1d = P(AXIS_NAME)
    spec_2d = P(AXIS_NAME, None)
    spec_3d = P(AXIS_NAME, None, None)
    in_specs = (spec_2d, spec_3d, spec_2d, spec_1d, spec_1d, spec_3d, spec_3d, spec_3d, spec_2d, spec_2d, spec_2d, spec_2d)
    out_specs = (spec_3d, spec_2d, spec_1d, spec_1d, spec_3d, spec_3d, spec_3d, spec_2d, spec_2d, spec_2d, spec_2d)

    def device_step(token_ids, grad_y, table, gain_one, gain_two, w_query, w_key, w_value, w_out, w_gate, w_up, w_down):
        me = lax.axis_index(AXIS_NAME)
        my_core, my_x, my_y = me % 2, me // 2 % 2, me // 4
        batch_loc, seq_len = token_ids.shape
        tokens = batch_loc * seq_len
        rows_dev, width = table.shape
        d_shard, ffn = w_gate.shape
        half = ffn // 2
        grad_own = grad_y.reshape(tokens, width)

        ids_all = lax.all_gather(token_ids.reshape(1, tokens), AXIS_NAME, axis=0, tiled=True)
        owner = ids_all // rows_dev
        place = jnp.arange(tokens, dtype=jnp.int32)
        same_id = ids_all[:, :, None] == ids_all[:, None, :]
        lead = jnp.min(jnp.where(same_id, place[None, None, :], tokens), axis=2)
        is_lead = lead == place[None, :]
        same_owner = owner[:, :, None] == owner[:, None, :]
        ahead = same_owner & is_lead[:, None, :] & (place[None, None, :] < lead[:, :, None])
        slot_fwd = jnp.sum(ahead.astype(jnp.int32), axis=2)
        earlier = same_owner & (place[None, None, :] < place[None, :, None])
        slot_bwd = jnp.sum(earlier.astype(jnp.int32), axis=2)
        owners = jnp.arange(N_DEV, dtype=jnp.int32)
        count_fwd = jnp.sum((is_lead[:, None, :] & (owner[:, None, :] == owners[None, :, None])).astype(jnp.int32), axis=2)
        count_bwd = jnp.sum((owner[:, None, :] == owners[None, :, None]).astype(jnp.int32), axis=2)
        fits = (jnp.max(count_fwd) <= SLOTS_FWD) & (jnp.max(count_bwd) <= SLOTS_BWD)
        mine = owner == me
        local = ids_all - me * rows_dev
        wanted_fwd = mine & is_lead
        peers = jnp.arange(N_DEV, dtype=jnp.int32) ^ me

        def table_of(slot, chosen, slots, fill):
            slot_p, chosen_p, local_p = (jnp.take(v, peers, axis=0) for v in (slot, chosen, local))
            hit = chosen_p[:, None, :] & (slot_p[:, None, :] == jnp.arange(slots, dtype=jnp.int32)[None, :, None])
            return jnp.max(jnp.where(hit, local_p[:, None, :], fill), axis=2)

        ask_rows = table_of(slot_fwd, wanted_fwd, SLOTS_FWD, 0)
        ask_count = jnp.minimum(jnp.take(jnp.take(count_fwd, me, axis=1), peers), SLOTS_FWD)
        grad_ids = table_of(slot_bwd, mine, SLOTS_BWD, -1).reshape(-1)
        grad_ids = jnp.where(grad_ids < 0, rows_dev, grad_ids)
        n_grad = N_DEV * SLOTS_BWD
        order = jnp.arange(n_grad, dtype=jnp.int32)
        before = (grad_ids[None, :] < grad_ids[:, None]) | ((grad_ids[None, :] == grad_ids[:, None]) & (order[None, :] < order[:, None]))
        rank = jnp.sum(before.astype(jnp.int32), axis=1)
        sorted_ids = jnp.max(jnp.where(rank[None, :] == order[:, None], grad_ids[None, :], 0), axis=1)
        own_owner = jnp.take(owner, me, axis=0)
        own_fwd = (own_owner ^ me) * SLOTS_FWD + jnp.take(slot_fwd, me, axis=0)
        own_bwd = (own_owner ^ me) * SLOTS_BWD + jnp.take(slot_bwd, me, axis=0)

        picked = pick_rows(table, ask_rows, ask_count)
        arrived = jnp.concatenate([picked[0]] + [swap(picked[r], r) for r in range(1, N_DEV)], axis=0)

        def rows_fast():
            hot = (own_fwd[:, None] == jnp.arange(N_DEV * SLOTS_FWD, dtype=jnp.int32)[None, :]).astype(BF16)
            return dot(hot, arrived).astype(BF16)

        def rows_any():
            parts = jnp.take(table, jnp.where(mine, local, 0).reshape(-1), axis=0)
            parts = jnp.where(mine.reshape(-1, 1), parts, jnp.zeros((), BF16))
            return lax.psum_scatter(parts, AXIS_NAME, scatter_dimension=0, tiled=True)

        emb_rows = lax.cond(fits, rows_fast, rows_any)

        def ffn_shard(w):
            v = w.reshape(d_shard, 2, 2, ffn // 4)
            keep = jnp.take(v, my_x, axis=2).reshape(d_shard, half)
            send = jnp.take(v, 1 - my_x, axis=2).reshape(d_shard, half)
            got = swap(send, BIT_X)
            a = jnp.concatenate([jnp.where(my_x == 0, keep, got), jnp.where(my_x == 0, got, keep)], axis=0)
            a_y = swap(a, BIT_Y)
            return jnp.concatenate([a, a_y, swap(a, BIT_CORE), swap(a_y, BIT_CORE)], axis=0)

        wg = ffn_shard(w_gate)
        wu = ffn_shard(w_up)
        wd_y = swap(w_down, BIT_Y)
        wd = jnp.zeros((2, 2) + w_down.shape, BF16)
        for c_rel, y_rel, piece in ((0, 0, w_down), (0, 1, wd_y), (1, 0, swap(w_down, BIT_CORE)), (1, 1, swap(wd_y, BIT_CORE))):
            wd = lax.dynamic_update_slice(wd, piece[None, None], (my_y ^ y_rel, my_core ^ c_rel, 0, 0))
        wd = wd.reshape(half, width)
        grad_nbr = swap(grad_own, BIT_X)

        gains = lax.all_gather(jnp.stack([gain_one, gain_two]), AXIS_NAME, axis=1, tiled=True)
        gain_one_f, gain_two_f = gains[0].astype(F32), gains[1].astype(F32)
        wq, wk, wv, wo = (lax.all_gather(w, AXIS_NAME, axis=0, tiled=True) for w in (w_query, w_key, w_value, w_out))
        emb_rows = emb_rows.reshape(batch_loc, seq_len, width)
        x_f32 = emb_rows.astype(F32)
        h_one, norm1_pull = jax.vjp(rms_norm, x_f32, gain_one_f)
        q_f32 = jnp.einsum("bsd,dhe->bshe", h_one, wq, preferred_element_type=F32)
        k_f32 = jnp.einsum("bsd,dhe->bshe", h_one, wk, preferred_element_type=F32)
        v_bf16 = jnp.einsum("bsd,dhe->bshe", h_one, wv, preferred_element_type=F32).astype(BF16)
        attn_out, attn_pull = jax.vjp(attend, q_f32, k_f32, v_bf16)
        resid_f32 = x_f32 + jnp.einsum("bse,ed->bsd", attn_out, wo, preferred_element_type=F32)
        resid_two = resid_f32.astype(BF16).astype(F32).reshape(tokens, width)
        h_two, norm2_pull = jax.vjp(rms_norm, resid_two, gain_two_f)

        def to_rel(h):
            v = h.reshape(tokens, 2, 2, 2, d_shard)
            parts = [
                lax.dynamic_slice(v, (0, my_y ^ y_rel, 0, my_core ^ c_rel, 0), (tokens, 1, 2, 1, d_shard)).reshape(tokens, 2 * d_shard)
                for c_rel in (0, 1)
                for y_rel in (0, 1)
            ]
            return jnp.concatenate(parts, axis=1)

        def from_rel(h):
            v = h.reshape(tokens, 2, 2, 2, d_shard)
            parts = [
                lax.dynamic_slice(v, (0, my_core ^ c_abs, my_y ^ y_abs, x_abs, 0), (tokens, 1, 1, 1, d_shard)).reshape(tokens, d_shard)
                for y_abs in (0, 1)
                for x_abs in (0, 1)
                for c_abs in (0, 1)
            ]
            return jnp.concatenate(parts, axis=1)

        h_own = to_rel(h_two)
        h_nbr = swap(h_own, BIT_X)

        def ffn_half(h, dy):
            gate_f32, up_f32 = dot(h, wg), dot(h, wu)
            act, act_pull = jax.vjp(gated, gate_f32, up_f32)
            d_act = dot_nt(dy, wd).astype(BF16)
            d_gate, d_up = act_pull(d_act)
            return act, d_gate.astype(BF16), d_up.astype(BF16)

        act_own, dg_own, du_own = ffn_half(h_own, grad_own)
        act_nbr, dg_nbr, du_nbr = ffn_half(h_nbr, grad_nbr)
        d_h_nbr = dot_nt(dg_nbr, wg) + dot_nt(du_nbr, wu)
        d_h_got = swap(d_h_nbr, BIT_X)
        y_nbr = dot(act_nbr, wd)
        y_got = swap(y_nbr, BIT_X)
        d_h_own = dot_nt(dg_own, wg) + dot_nt(du_own, wu)
        y_own = dot(act_own, wd)
        layer_out = (resid_two + (y_own + y_got)).astype(BF16)
        d_h_two = from_rel((d_h_own + d_h_got).astype(BF16))

        def two_stage(left, right):
            n = left.shape[1] // 4
            part = lambda c, y: dot_tn(left[:, (2 * c + y) * n : (2 * c + y + 1) * n], right)
            far = part(0, 1) + swap(part(1, 1), BIT_CORE)
            got = swap(far, BIT_Y)
            near = part(0, 0) + swap(part(1, 0), BIT_CORE)
            return (near + got).astype(BF16)

        def act_rel(a):
            v = a.reshape(tokens, 2, 2, half // 4)
            return [
                lax.dynamic_slice(v, (0, my_y ^ y_rel, my_core ^ c_rel, 0), (tokens, 1, 1, half // 4)).reshape(tokens, half // 4)
                for c_rel in (0, 1)
                for y_rel in (0, 1)
            ]

        act_both = jnp.concatenate([jnp.concatenate(act_rel(act_own), axis=1), jnp.concatenate(act_rel(act_nbr), axis=1)], axis=0)
        dy_both = jnp.concatenate([grad_own, grad_nbr], axis=0)
        h_both = jnp.concatenate([h_own, h_nbr], axis=0)
        dg_both = jnp.concatenate([dg_own, dg_nbr], axis=0)
        du_both = jnp.concatenate([du_own, du_nbr], axis=0)
        g_down = two_stage(act_both, dy_both)

        def finish(g):
            v = g.reshape(2, d_shard, half)
            keep = jnp.take(v, my_x, axis=0)
            got = swap(jnp.take(v, 1 - my_x, axis=0), BIT_X)
            keep, got = keep.reshape(d_shard, 2, 1, ffn // 4), got.reshape(d_shard, 2, 1, ffn // 4)
            lo, hi = jnp.where(my_x == 0, keep, got), jnp.where(my_x == 0, got, keep)
            return jnp.concatenate([lo, hi], axis=2).reshape(d_shard, ffn)

        g_gate = finish(two_stage(h_both, dg_both))
        g_up = finish(two_stage(h_both, du_both))

        d_resid_two, g_norm2 = norm2_pull(d_h_two)
        d_resid = (grad_own.astype(F32) + d_resid_two).astype(BF16).reshape(batch_loc, seq_len, width)
        g_out = jnp.einsum("bse,bsd->ed", attn_out, d_resid, preferred_element_type=F32)
        d_attn = jnp.einsum("bsd,ed->bse", d_resid, wo, preferred_element_type=F32).astype(BF16)
        d_query, d_key, d_value = attn_pull(d_attn)
        d_query = d_query.astype(BF16)
        d_key = d_key.astype(BF16)
        d_h_one = (
            jnp.einsum("bshe,dhe->bsd", d_query, wq, preferred_element_type=F32)
            + jnp.einsum("bshe,dhe->bsd", d_key, wk, preferred_element_type=F32)
            + jnp.einsum("bshe,dhe->bsd", d_value, wv, preferred_element_type=F32)
        ).astype(BF16)
        d_x, g_norm1 = norm1_pull(d_h_one)
        d_emb = (d_resid.astype(F32) + d_x).astype(BF16).reshape(tokens, width)

        hot_bwd = (own_bwd[:, None] == jnp.arange(n_grad, dtype=jnp.int32)[None, :]).astype(BF16)
        outgoing = dot_tn(hot_bwd, d_emb).astype(BF16).reshape(N_DEV, SLOTS_BWD, width)
        incoming = jnp.concatenate([outgoing[0]] + [swap(outgoing[r], r) for r in range(1, N_DEV)], axis=0)

        g_query = jnp.einsum("bsd,bshe->dhe", h_one, d_query, preferred_element_type=F32)
        g_key = jnp.einsum("bsd,bshe->dhe", h_one, d_key, preferred_element_type=F32)
        g_value = jnp.einsum("bsd,bshe->dhe", h_one, d_value, preferred_element_type=F32)
        scatter = lambda g: lax.psum_scatter(g, AXIS_NAME, scatter_dimension=0, tiled=True).astype(BF16)
        g_out, g_query, g_key, g_value, g_norm1, g_norm2 = (scatter(g) for g in (g_out, g_query, g_key, g_value, g_norm1, g_norm2))

        def grad_fast():
            to_sorted = (rank[None, :] == order[:, None]).astype(BF16)
            return table_grad(sorted_ids, dot(to_sorted, incoming).astype(BF16), rows_dev)

        def grad_any():
            d_all = lax.all_gather(d_emb, AXIS_NAME, axis=0, tiled=True).astype(F32)
            return jax.ops.segment_sum(d_all, jnp.where(mine, local, rows_dev).reshape(-1), num_segments=rows_dev).astype(BF16)

        d_table = lax.cond(fits, grad_fast, grad_any)
        return layer_out.reshape(batch_loc, seq_len, width), d_table, g_norm1, g_norm2, g_query, g_key, g_value, g_out, g_gate, g_up, g_down

    return jax.shard_map(device_step, mesh=mesh, in_specs=in_specs, out_specs=out_specs, check_vma=False)
```
